8 devices in a mesh: mp: 2 (over z, y), dp: 4 (over x, core).
Axes of the slice: x: 2, y: 2, z: 1, core: 2. Of those that a mesh axis runs over, the one named last changes fastest.
Arguments:
- a_mat: bfloat16 [2048, 98304], P(('mp', 'dp'))
- b_mat: bfloat16 [98304, 5632], P(('mp', 'dp'))
Outputs:
- output: bfloat16 [2048, 5632], P(('mp', 'dp'))
All inputs are finite; a program needn't handle non-finite values.
Results may differ from the reference program's by a relative error of at most 0.001.
Values are sent between devices in bfloat16 or wider.
A program may use at most 1 GiB of HBM per device.

```python
import jax
import jax.numpy as jnp

M_DIM = 2048
N_DIM = 5632
TOKENS = 98304


def setup_inputs(seed: int = 0) -> dict:
    root_key = jax.random.key(seed)
    key_a, key_b = jax.random.split(root_key)
    a_mat = jax.random.normal(key_a, (M_DIM, TOKENS), jnp.float32)
    b_mat = jax.random.normal(key_b, (TOKENS, N_DIM), jnp.float32) * (TOKENS ** -0.5)
    return {"a_mat": a_mat.astype(jnp.bfloat16), "b_mat": b_mat.astype(jnp.bfloat16)}


def reference(a_mat, b_mat):
    return jnp.dot(a_mat, b_mat, preferred_element_type=jnp.float32).astype(jnp.bfloat16)
```

```python
import jax
import jax.numpy as jnp
from jax import lax
from jax.experimental import pallas as pl
from jax.experimental.pallas import tpu as pltpu
from jax.sharding import PartitionSpec as P

MESH = pl.DeviceIdType.MESH
PEERS = ((1, 0, 0), (0, 1, 0), (1, 1, 0), (1, 0, 1), (0, 1, 1), (1, 1, 1), (0, 0, 1))
CHUNKS = 4
COLS = 512
PIECE = 2048
DEPTH = 4096
AHEAD = 1
LAG1 = 2
LAG2 = 2
SUMS1, SUMS2 = LAG1 + 2, LAG2 + 2
SLOTS1, SLOTS2 = 2 * LAG1 + 2, 2 * LAG2 + 2


def kernel(
    a_ref, b_ref, c_ref, g_ref,
    a_v, b_v, p_v, rd_v, s1_v, r1_v, s2_v, r2_v, o_v,
    a_send, a_recv, a_load, b_load, d_send, d_recv, s1_send, r1_recv, s2_send, r2_recv, o_sem,
):
    _, _, rows, k_dim = g_ref.shape
    half = 4 * rows
    blocks = b_ref.shape[1] // COLS
    pieces = k_dim // PIECE
    steps = CHUNKS * blocks

    y = lax.axis_index("mp")
    x = lax.axis_index("dp") // 2
    c = lax.axis_index("dp") % 2
    f = (1 - c) * x + c * y
    g = (1 - c) * y + c * x
    first = ((1 - c) * y + c * (1 - y), ((1 - c) * (1 - x) + c * x) * 2 + c)
    second = ((1 - c) * (1 - y) + c * y, ((1 - c) * x + c * (1 - x)) * 2 + c)
    sibling = (y, x * 2 + 1 - c)
    me = (y * 2 + x) * 2 + c
    my_pos = 4 * c + 2 * f + g

    def peer(i):
        dx, dy, dc = PEERS[i]
        px, py, pc = (x + dx) % 2, (y + dy) % 2, (c + dc) % 2
        pos = 4 * pc + (1 - pc) * (2 * px + py) + pc * (2 * py + px)
        return (py, px * 2 + pc), (py * 2 + px) * 2 + pc, pos

    def a_rows(j):
        return pl.ds(pl.multiple_of(j * rows, rows), rows)

    def a_copy(i, j, start, size):
        device, index, _ = peer(i)
        return pltpu.make_async_remote_copy(
            src_ref=a_ref.at[a_rows(j), pl.ds(pl.multiple_of(index * k_dim + start, 128), size)],
            dst_ref=g_ref.at[j, my_pos, :, pl.ds(pl.multiple_of(start, 128), size)],
            send_sem=a_send.at[j, i],
            recv_sem=a_recv.at[j, i],
            device_id=device,
            device_id_type=MESH,
        )

    def send_piece(u):
        for i in range(len(PEERS)):
            a_copy(i, u // pieces, (u % pieces) * PIECE, PIECE).start()

    def a_loads(j):
        copies = []
        for i in range(len(PEERS)):
            _, _, pos = peer(i)
            copies.append(pltpu.make_async_copy(
                g_ref.at[j, pos], a_v.at[pl.ds(pl.multiple_of(pos * rows, rows), rows), :], a_load.at[i]
            ))
        copies.append(pltpu.make_async_copy(
            a_ref.at[a_rows(j), pl.ds(pl.multiple_of(me * k_dim, 128), k_dim)],
            a_v.at[pl.ds(pl.multiple_of(my_pos * rows, rows), rows), :],
            a_load.at[len(PEERS)],
        ))
        return copies

    def b_copy(s):
        return pltpu.make_async_copy(
            b_ref.at[:, pl.ds(pl.multiple_of((s % blocks) * COLS, COLS), COLS)], b_v.at[s % 2], b_load.at[s % 2]
        )

    def d_copy(b):
        return pltpu.make_async_remote_copy(
            src_ref=p_v.at[b % 2, pl.ds(pl.multiple_of((1 - c) * half, half), half), :],
            dst_ref=rd_v.at[b % 2],
            send_sem=d_send.at[b % 2],
            recv_sem=d_recv.at[b % 2],
            device_id=sibling,
            device_id_type=MESH,
        )

    def first_copy(b):
        return pltpu.make_async_remote_copy(
            src_ref=s1_v.at[b % SUMS1, pl.ds(pl.multiple_of((1 - f) * 2 * rows, 2 * rows), 2 * rows), :],
            dst_ref=r1_v.at[b % SLOTS1],
            send_sem=s1_send.at[b % SUMS1],
            recv_sem=r1_recv.at[b % SLOTS1],
            device_id=first,
            device_id_type=MESH,
        )

    def second_copy(b):
        return pltpu.make_async_remote_copy(
            src_ref=s2_v.at[b % SUMS2, pl.ds(pl.multiple_of((1 - g) * rows, rows), rows), :],
            dst_ref=r2_v.at[b % SLOTS2],
            send_sem=s2_send.at[b % SUMS2],
            recv_sem=r2_recv.at[b % SLOTS2],
            device_id=second,
            device_id_type=MESH,
        )

    def out_copy(b):
        return pltpu.make_async_copy(
            o_v.at[b % 2],
            c_ref.at[a_rows(b // blocks), pl.ds(pl.multiple_of((b % blocks) * COLS, COLS), COLS)],
            o_sem.at[b % 2],
        )

    def valid(b):
        return jnp.logical_and(b >= 0, b < steps)

    b_copy(0).start()
    barrier = pltpu.get_barrier_semaphore()
    for i in range(len(PEERS)):
        pl.semaphore_signal(barrier, inc=1, device_id=peer(i)[0], device_id_type=MESH)
    pl.semaphore_wait(barrier, len(PEERS))

    @pl.loop(0, pieces + AHEAD)
    def _(u):
        send_piece(u)

    @pl.loop(0, steps + 3 + LAG1 + LAG2)
    def _(s):
        j, n = s // blocks, s % blocks

        @pl.when(s + 1 < steps)
        def _():
            b_copy(s + 1).start()

        @pl.when(valid(s - 1))
        def _():
            d_copy(s - 1).start()

        @pl.when(valid(s - 2))
        def _():
            first_copy(s - 2).start()

        @pl.when(valid(s - 3 - LAG1))
        def _():
            second_copy(s - 3 - LAG1).start()

        unit = (j + 1) * pieces + n // 2 + AHEAD

        @pl.when(jnp.logical_and(n % 2 == 0, unit < CHUNKS * pieces))
        def _():
            send_piece(unit)

        @pl.when(s < steps)
        def _():
            @pl.when(n == 0)
            def _():
                for i in range(len(PEERS)):
                    a_copy(i, j, 0, k_dim).wait_recv()
                loads = a_loads(j)
                for load in loads:
                    load.start()
                for load in loads:
                    load.wait()

            b_copy(s).wait()

            @pl.loop(0, k_dim // DEPTH)
            def _(k):
                part = pl.ds(pl.multiple_of(k * DEPTH, DEPTH), DEPTH)
                dot = jnp.dot(a_v[:, part], b_v[s % 2, part, :], preferred_element_type=jnp.float32)

                @pl.when(k == 0)
                def _():
                    p_v[s % 2] = dot

                @pl.when(k > 0)
                def _():
                    p_v[s % 2] += dot

        @pl.when(valid(s - 1))
        def _():
            b = s - 1
            d_copy(b).wait_recv()
            s1_v[b % SUMS1] = p_v[b % 2, pl.ds(pl.multiple_of(c * half, half), half), :] + rd_v[b % 2]
            d_copy(b).wait_send()

        @pl.when(valid(s - 2 - LAG1))
        def _():
            b = s - 2 - LAG1
            first_copy(b).wait_recv()
            kept = s1_v[b % SUMS1, pl.ds(pl.multiple_of(f * 2 * rows, 2 * rows), 2 * rows), :]
            s2_v[b % SUMS2] = kept + r1_v[b % SLOTS1]
            first_copy(b).wait_send()

        @pl.when(valid(s - 3 - LAG1 - LAG2))
        def _():
            b = s - 3 - LAG1 - LAG2

            @pl.when(b >= 2)
            def _():
                out_copy(b - 2).wait()

            second_copy(b).wait_recv()
            kept = s2_v[b % SUMS2, pl.ds(pl.multiple_of(g * rows, rows), rows), :]
            o_v[b % 2] = (kept + r2_v[b % SLOTS2]).astype(o_v.dtype)
            second_copy(b).wait_send()
            out_copy(b).start()

    out_copy(steps - 2).wait()
    out_copy(steps - 1).wait()

    @pl.loop(0, CHUNKS)
    def _(j):
        for i in range(len(PEERS)):
            a_copy(i, j, 0, k_dim).wait_send()


def solution(mesh):
    def local_product(a_rows, b_rows):
        row_count = a_rows.shape[0]
        k_dim, n_dim = b_rows.shape
        rows = row_count // CHUNKS
        f32, dma = jnp.float32, pltpu.SemaphoreType.DMA
        c_rows, _ = pl.pallas_call(
            kernel,
            name="exchange_matmul",
            out_shape=(
                jax.ShapeDtypeStruct((row_count, n_dim), jnp.bfloat16),
                jax.ShapeDtypeStruct((CHUNKS, 8, rows, k_dim), jnp.bfloat16),
            ),
            in_specs=[pl.BlockSpec(memory_space=pl.ANY)] * 2,
            out_specs=[pl.BlockSpec(memory_space=pl.ANY)] * 2,
            scratch_shapes=[
                pltpu.VMEM((8 * rows, k_dim), jnp.bfloat16),
                pltpu.VMEM((2, k_dim, COLS), jnp.bfloat16),
                pltpu.VMEM((2, 8 * rows, COLS), f32),
                pltpu.VMEM((2, 4 * rows, COLS), f32),
                pltpu.VMEM((SUMS1, 4 * rows, COLS), f32),
                pltpu.VMEM((SLOTS1, 2 * rows, COLS), f32),
                pltpu.VMEM((SUMS2, 2 * rows, COLS), f32),
                pltpu.VMEM((SLOTS2, rows, COLS), f32),
                pltpu.VMEM((2, rows, COLS), jnp.bfloat16),
                dma((CHUNKS, len(PEERS))),
                dma((CHUNKS, len(PEERS))),
                dma((len(PEERS) + 1,)),
                dma((2,)),
                dma((2,)),
                dma((2,)),
                dma((SUMS1,)),
                dma((SLOTS1,)),
                dma((SUMS2,)),
                dma((SLOTS2,)),
                dma((2,)),
            ],
            compiler_params=pltpu.CompilerParams(
                collective_id=0, has_side_effects=True, vmem_limit_bytes=62 * 1024 * 1024
            ),
            cost_estimate=pl.CostEstimate(
                flops=2 * 8 * row_count * k_dim * n_dim,
                bytes_accessed=2 * CHUNKS * k_dim * n_dim,
                transcendentals=0,
            ),
        )(a_rows, b_rows)
        return c_rows

    return jax.shard_map(
        local_product,
        mesh=mesh,
        in_specs=(P(("mp", "dp"), None), P(("mp", "dp"), None)),
        out_specs=P(("mp", "dp"), None),
        check_vma=False,
    )
```

```python
import jax
import jax.numpy as jnp
from jax import lax
from jax.experimental import pallas as pl
from jax.experimental.pallas import tpu as pltpu
from jax.sharding import PartitionSpec as P

MESH = pl.DeviceIdType.MESH
PEERS = ((1, 0, 0), (0, 1, 0), (1, 1, 0), (1, 0, 1), (0, 1, 1), (1, 1, 1), (0, 0, 1))
CHUNKS = 8
COLS = 512
PIECE = 2048
AHEAD = 2
LAG1 = 3
LAG2 = 3
SUMS1, SUMS2 = LAG1 + 2, LAG2 + 2
SLOTS1, SLOTS2 = 2 * LAG1 + 2, 2 * LAG2 + 2


def kernel(
    a_ref, b_ref, c_ref, g_ref,
    a_v, b_v, p_v, rd_v, s1_v, r1_v, s2_v, r2_v, o_v,
    a_send, a_recv, a_load, b_load, d_send, d_recv, s1_send, r1_recv, s2_send, r2_recv, o_sem,
):
    _, _, rows, k_dim = g_ref.shape
    half = 4 * rows
    blocks = b_ref.shape[1] // COLS
    pieces = k_dim // PIECE
    steps = CHUNKS * blocks

    y = lax.axis_index("mp")
    x = lax.axis_index("dp") // 2
    c = lax.axis_index("dp") % 2
    f = (1 - c) * x + c * y
    g = (1 - c) * y + c * x
    first = ((1 - c) * y + c * (1 - y), ((1 - c) * (1 - x) + c * x) * 2 + c)
    second = ((1 - c) * (1 - y) + c * y, ((1 - c) * x + c * (1 - x)) * 2 + c)
    sibling = (y, x * 2 + 1 - c)
    me = (y * 2 + x) * 2 + c
    my_pos = 4 * c + 2 * f + g

    def peer(i):
        dx, dy, dc = PEERS[i]
        px, py, pc = (x + dx) % 2, (y + dy) % 2, (c + dc) % 2
        pos = 4 * pc + (1 - pc) * (2 * px + py) + pc * (2 * py + px)
        return (py, px * 2 + pc), (py * 2 + px) * 2 + pc, pos

    def a_rows(j):
        return pl.ds(pl.multiple_of(j * rows, rows), rows)

    def a_copy(i, j, start, size):
        device, index, _ = peer(i)
        return pltpu.make_async_remote_copy(
            src_ref=a_ref.at[a_rows(j), pl.ds(pl.multiple_of(index * k_dim + start, 128), size)],
            dst_ref=g_ref.at[j, my_pos, :, pl.ds(pl.multiple_of(start, 128), size)],
            send_sem=a_send.at[j, i],
            recv_sem=a_recv.at[j, i],
            device_id=device,
            device_id_type=MESH,
        )

    def send_piece(u):
        for i in range(len(PEERS)):
            a_copy(i, u // pieces, (u % pieces) * PIECE, PIECE).start()

    def a_loads(j):
        copies = []
        for i in range(len(PEERS)):
            _, _, pos = peer(i)
            copies.append(pltpu.make_async_copy(
                g_ref.at[j, pos], a_v.at[pl.ds(pl.multiple_of(pos * rows, rows), rows), :], a_load.at[i]
            ))
        copies.append(pltpu.make_async_copy(
            a_ref.at[a_rows(j), pl.ds(pl.multiple_of(me * k_dim, 128), k_dim)],
            a_v.at[pl.ds(pl.multiple_of(my_pos * rows, rows), rows), :],
            a_load.at[len(PEERS)],
        ))
        return copies

    def b_copy(s):
        return pltpu.make_async_copy(
            b_ref.at[:, pl.ds(pl.multiple_of((s % blocks) * COLS, COLS), COLS)], b_v.at[s % 2], b_load.at[s % 2]
        )

    def d_copy(b):
        return pltpu.make_async_remote_copy(
            src_ref=p_v.at[b % 2, pl.ds(pl.multiple_of((1 - c) * half, half), half), :],
            dst_ref=rd_v.at[b % 2],
            send_sem=d_send.at[b % 2],
            recv_sem=d_recv.at[b % 2],
            device_id=sibling,
            device_id_type=MESH,
        )

    def first_copy(b):
        return pltpu.make_async_remote_copy(
            src_ref=s1_v.at[b % SUMS1, pl.ds(pl.multiple_of((1 - f) * 2 * rows, 2 * rows), 2 * rows), :],
            dst_ref=r1_v.at[b % SLOTS1],
            send_sem=s1_send.at[b % SUMS1],
            recv_sem=r1_recv.at[b % SLOTS1],
            device_id=first,
            device_id_type=MESH,
        )

    def second_copy(b):
        return pltpu.make_async_remote_copy(
            src_ref=s2_v.at[b % SUMS2, pl.ds(pl.multiple_of((1 - g) * rows, rows), rows), :],
            dst_ref=r2_v.at[b % SLOTS2],
            send_sem=s2_send.at[b % SUMS2],
            recv_sem=r2_recv.at[b % SLOTS2],
            device_id=second,
            device_id_type=MESH,
        )

    def out_copy(b):
        return pltpu.make_async_copy(
            o_v.at[b % 2],
            c_ref.at[a_rows(b // blocks), pl.ds(pl.multiple_of((b % blocks) * COLS, COLS), COLS)],
            o_sem.at[b % 2],
        )

    def valid(b):
        return jnp.logical_and(b >= 0, b < steps)

    b_copy(0).start()
    barrier = pltpu.get_barrier_semaphore()
    for i in range(len(PEERS)):
        pl.semaphore_signal(barrier, inc=1, device_id=peer(i)[0], device_id_type=MESH)
    pl.semaphore_wait(barrier, len(PEERS))

    @pl.loop(0, pieces + AHEAD)
    def _(u):
        send_piece(u)

    @pl.loop(0, steps + 3 + LAG1 + LAG2)
    def _(s):
        j, n = s // blocks, s % blocks

        @pl.when(s + 1 < steps)
        def _():
            b_copy(s + 1).start()

        @pl.when(valid(s - 1))
        def _():
            d_copy(s - 1).start()

        @pl.when(valid(s - 2))
        def _():
            first_copy(s - 2).start()

        @pl.when(valid(s - 3 - LAG1))
        def _():
            second_copy(s - 3 - LAG1).start()

        unit = (j + 1) * pieces + n // 2 + AHEAD

        @pl.when(jnp.logical_and(n % 2 == 0, unit < CHUNKS * pieces))
        def _():
            send_piece(unit)

        @pl.when(s < steps)
        def _():
            @pl.when(n == 0)
            def _():
                for i in range(len(PEERS)):
                    a_copy(i, j, 0, k_dim).wait_recv()
                loads = a_loads(j)
                for load in loads:
                    load.start()
                for load in loads:
                    load.wait()

            b_copy(s).wait()

            p_v[s % 2] = jnp.dot(a_v[...], b_v[s % 2], preferred_element_type=jnp.float32)

        @pl.when(valid(s - 1))
        def _():
            b = s - 1
            d_copy(b).wait_recv()
            s1_v[b % SUMS1] = p_v[b % 2, pl.ds(pl.multiple_of(c * half, half), half), :] + rd_v[b % 2]
            d_copy(b).wait_send()

        @pl.when(valid(s - 2 - LAG1))
        def _():
            b = s - 2 - LAG1
            first_copy(b).wait_recv()
            kept = s1_v[b % SUMS1, pl.ds(pl.multiple_of(f * 2 * rows, 2 * rows), 2 * rows), :]
            s2_v[b % SUMS2] = kept + r1_v[b % SLOTS1]
            first_copy(b).wait_send()

        @pl.when(valid(s - 3 - LAG1 - LAG2))
        def _():
            b = s - 3 - LAG1 - LAG2

            @pl.when(b >= 2)
            def _():
                out_copy(b - 2).wait()

            second_copy(b).wait_recv()
            kept = s2_v[b % SUMS2, pl.ds(pl.multiple_of(g * rows, rows), rows), :]
            o_v[b % 2] = (kept + r2_v[b % SLOTS2]).astype(o_v.dtype)
            second_copy(b).wait_send()
            out_copy(b).start()

    out_copy(steps - 2).wait()
    out_copy(steps - 1).wait()

    @pl.loop(0, CHUNKS)
    def _(j):
        for i in range(len(PEERS)):
            a_copy(i, j, 0, k_dim).wait_send()


def solution(mesh):
    def local_product(a_rows, b_rows):
        row_count = a_rows.shape[0]
        k_dim, n_dim = b_rows.shape
        rows = row_count // CHUNKS
        f32, dma = jnp.float32, pltpu.SemaphoreType.DMA
        c_rows, _ = pl.pallas_call(
            kernel,
            name="exchange_matmul",
            out_shape=(
                jax.ShapeDtypeStruct((row_count, n_dim), jnp.bfloat16),
                jax.ShapeDtypeStruct((CHUNKS, 8, rows, k_dim), jnp.bfloat16),
            ),
            in_specs=[pl.BlockSpec(memory_space=pl.ANY)] * 2,
            out_specs=[pl.BlockSpec(memory_space=pl.ANY)] * 2,
            scratch_shapes=[
                pltpu.VMEM((8 * rows, k_dim), jnp.bfloat16),
                pltpu.VMEM((2, k_dim, COLS), jnp.bfloat16),
                pltpu.VMEM((2, 8 * rows, COLS), f32),
                pltpu.VMEM((2, 4 * rows, COLS), f32),
                pltpu.VMEM((SUMS1, 4 * rows, COLS), f32),
                pltpu.VMEM((SLOTS1, 2 * rows, COLS), f32),
                pltpu.VMEM((SUMS2, 2 * rows, COLS), f32),
                pltpu.VMEM((SLOTS2, rows, COLS), f32),
                pltpu.VMEM((2, rows, COLS), jnp.bfloat16),
                dma((CHUNKS, len(PEERS))),
                dma((CHUNKS, len(PEERS))),
                dma((len(PEERS) + 1,)),
                dma((2,)),
                dma((2,)),
                dma((2,)),
                dma((SUMS1,)),
                dma((SLOTS1,)),
                dma((SUMS2,)),
                dma((SLOTS2,)),
                dma((2,)),
            ],
            compiler_params=pltpu.CompilerParams(
                collective_id=0, has_side_effects=True, vmem_limit_bytes=62 * 1024 * 1024
            ),
            cost_estimate=pl.CostEstimate(
                flops=2 * 8 * row_count * k_dim * n_dim,
                bytes_accessed=2 * CHUNKS * k_dim * n_dim,
                transcendentals=0,
            ),
        )(a_rows, b_rows)
        return c_rows

    return jax.shard_map(
        local_product,
        mesh=mesh,
        in_specs=(P(("mp", "dp"), None), P(("mp", "dp"), None)),
        out_specs=P(("mp", "dp"), None),
        check_vma=False,
    )
```

```python
import functools

import jax
import jax.numpy as jnp
from jax import lax
from jax.experimental import pallas as pl
from jax.experimental.pallas import tpu as pltpu
from jax.sharding import PartitionSpec as P

MESH = pl.DeviceIdType.MESH
PEERS = ((1, 0, 0), (0, 1, 0), (1, 1, 0), (1, 0, 1), (0, 1, 1), (1, 1, 1), (0, 0, 1))
CHUNKS = 8
COLS = 512
PIECE = 2048
AHEAD = 2
HELD = 12
BURST = 2
LAG1 = 4
LAG2 = 4
SUMS1, SUMS2 = HELD + LAG1 + 3, BURST * (LAG2 + 2)
SLOTS1, SLOTS2 = BURST * (2 * LAG1 + 2), BURST * (2 * LAG2 + 2)


def kernel(
    a_ref, b_ref, c_ref, g_ref,
    a_v, b_v, p_v, rd_v, s1_v, r1_v, s2_v, r2_v, o_v,
    a_send, a_recv, a_load, b_load, d_send, d_recv, s1_send, r1_recv, s2_send, r2_recv, o_sem,
):
    _, _, rows, k_dim = g_ref.shape
    half = 4 * rows
    blocks = b_ref.shape[1] // COLS
    pieces = k_dim // PIECE
    steps = CHUNKS * blocks

    y = lax.axis_index("mp")
    x = lax.axis_index("dp") // 2
    c = lax.axis_index("dp") % 2
    f = (1 - c) * x + c * y
    g = (1 - c) * y + c * x
    first = ((1 - c) * y + c * (1 - y), ((1 - c) * (1 - x) + c * x) * 2 + c)
    second = ((1 - c) * (1 - y) + c * y, ((1 - c) * x + c * (1 - x)) * 2 + c)
    sibling = (y, x * 2 + 1 - c)
    me = (y * 2 + x) * 2 + c
    my_pos = 4 * c + 2 * f + g

    def peer(i):
        dx, dy, dc = PEERS[i]
        px, py, pc = (x + dx) % 2, (y + dy) % 2, (c + dc) % 2
        pos = 4 * pc + (1 - pc) * (2 * px + py) + pc * (2 * py + px)
        return (py, px * 2 + pc), (py * 2 + px) * 2 + pc, pos

    def a_rows(j):
        return pl.ds(pl.multiple_of(j * rows, rows), rows)

    def a_copy(i, j, start, size):
        device, index, _ = peer(i)
        return pltpu.make_async_remote_copy(
            src_ref=a_ref.at[a_rows(j), pl.ds(pl.multiple_of(index * k_dim + start, 128), size)],
            dst_ref=g_ref.at[j, my_pos, :, pl.ds(pl.multiple_of(start, 128), size)],
            send_sem=a_send.at[j, i],
            recv_sem=a_recv.at[j, i],
            device_id=device,
            device_id_type=MESH,
        )

    def send_piece(u):
        for i in range(len(PEERS)):
            a_copy(i, u // pieces, (u % pieces) * PIECE, PIECE).start()

    def a_loads(j):
        copies = []
        for i in range(len(PEERS)):
            _, _, pos = peer(i)
            copies.append(pltpu.make_async_copy(
                g_ref.at[j, pos], a_v.at[pl.ds(pl.multiple_of(pos * rows, rows), rows), :], a_load.at[i]
            ))
        copies.append(pltpu.make_async_copy(
            a_ref.at[a_rows(j), pl.ds(pl.multiple_of(me * k_dim, 128), k_dim)],
            a_v.at[pl.ds(pl.multiple_of(my_pos * rows, rows), rows), :],
            a_load.at[len(PEERS)],
        ))
        return copies

    def b_copy(s):
        return pltpu.make_async_copy(
            b_ref.at[:, pl.ds(pl.multiple_of((s % blocks) * COLS, COLS), COLS)], b_v.at[s % 2], b_load.at[s % 2]
        )

    def d_copy(b):
        return pltpu.make_async_remote_copy(
            src_ref=p_v.at[b % 2, pl.ds(pl.multiple_of((1 - c) * half, half), half), :],
            dst_ref=rd_v.at[b % 2],
            send_sem=d_send.at[b % 2],
            recv_sem=d_recv.at[b % 2],
            device_id=sibling,
            device_id_type=MESH,
        )

    def first_copy(b):
        return pltpu.make_async_remote_copy(
            src_ref=s1_v.at[b % SUMS1, pl.ds(pl.multiple_of((1 - f) * 2 * rows, 2 * rows), 2 * rows), :],
            dst_ref=r1_v.at[b % SLOTS1],
            send_sem=s1_send.at[b % SUMS1],
            recv_sem=r1_recv.at[b % SLOTS1],
            device_id=first,
            device_id_type=MESH,
        )

    def second_copy(b):
        return pltpu.make_async_remote_copy(
            src_ref=s2_v.at[b % SUMS2, pl.ds(pl.multiple_of((1 - g) * rows, rows), rows), :],
            dst_ref=r2_v.at[b % SLOTS2],
            send_sem=s2_send.at[b % SUMS2],
            recv_sem=r2_recv.at[b % SLOTS2],
            device_id=second,
            device_id_type=MESH,
        )

    def out_copy(b):
        return pltpu.make_async_copy(
            o_v.at[b % 2],
            c_ref.at[a_rows(b // blocks), pl.ds(pl.multiple_of((b % blocks) * COLS, COLS), COLS)],
            o_sem.at[b % 2],
        )

    def valid(b):
        return jnp.logical_and(b >= 0, b < steps)

    catch_up = steps - max(blocks, HELD)

    def sent(s):
        extra = jnp.maximum(s - catch_up + 1, 0) * (BURST - 1)
        return jnp.clip(jnp.minimum(s - 1, s - 1 - HELD + extra), 0, steps)

    def each(low, high, body):
        for i in range(BURST):
            pl.when(low + i < high)(functools.partial(body, low + i))

    b_copy(0).start()
    barrier = pltpu.get_barrier_semaphore()
    for i in range(len(PEERS)):
        pl.semaphore_signal(barrier, inc=1, device_id=peer(i)[0], device_id_type=MESH)
    pl.semaphore_wait(barrier, len(PEERS))

    @pl.loop(0, pieces + AHEAD)
    def _(u):
        send_piece(u)

    @pl.loop(0, steps + 3 + LAG1 + LAG2)
    def _(s):
        j, n = s // blocks, s % blocks

        @pl.when(s + 1 < steps)
        def _():
            b_copy(s + 1).start()

        @pl.when(valid(s - 1))
        def _():
            d_copy(s - 1).start()

        each(sent(s - 1), sent(s), lambda b: first_copy(b).start())
        each(sent(s - 2 - LAG1), sent(s - 1 - LAG1), lambda b: second_copy(b).start())

        unit = (j + 1) * pieces + n // 2 + AHEAD

        @pl.when(jnp.logical_and(n % 2 == 0, unit < CHUNKS * pieces))
        def _():
            send_piece(unit)

        @pl.when(s < steps)
        def _():
            @pl.when(n == 0)
            def _():
                for i in range(len(PEERS)):
                    a_copy(i, j, 0, k_dim).wait_recv()
                loads = a_loads(j)
                for load in loads:
                    load.start()
                for load in loads:
                    load.wait()

            b_copy(s).wait()

            p_v[s % 2] = jnp.dot(a_v[...], b_v[s % 2], preferred_element_type=jnp.float32)

        @pl.when(valid(s - 1))
        def _():
            b = s - 1
            d_copy(b).wait_recv()
            s1_v[b % SUMS1] = p_v[b % 2, pl.ds(pl.multiple_of(c * half, half), half), :] + rd_v[b % 2]
            d_copy(b).wait_send()

        def add_first(b):
            first_copy(b).wait_recv()
            kept = s1_v[b % SUMS1, pl.ds(pl.multiple_of(f * 2 * rows, 2 * rows), 2 * rows), :]
            s2_v[b % SUMS2] = kept + r1_v[b % SLOTS1]
            first_copy(b).wait_send()

        def add_second(b):
            @pl.when(b >= 2)
            def _():
                out_copy(b - 2).wait()

            second_copy(b).wait_recv()
            kept = s2_v[b % SUMS2, pl.ds(pl.multiple_of(g * rows, rows), rows), :]
            o_v[b % 2] = (kept + r2_v[b % SLOTS2]).astype(o_v.dtype)
            second_copy(b).wait_send()
            out_copy(b).start()

        each(sent(s - 1 - LAG1), sent(s - LAG1), add_first)
        each(sent(s - 2 - LAG1 - LAG2), sent(s - 1 - LAG1 - LAG2), add_second)

    out_copy(steps - 2).wait()
    out_copy(steps - 1).wait()

    @pl.loop(0, CHUNKS)
    def _(j):
        for i in range(len(PEERS)):
            a_copy(i, j, 0, k_dim).wait_send()


def solution(mesh):
    def local_product(a_rows, b_rows):
        row_count = a_rows.shape[0]
        k_dim, n_dim = b_rows.shape
        rows = row_count // CHUNKS
        f32, dma = jnp.float32, pltpu.SemaphoreType.DMA
        c_rows, _ = pl.pallas_call(
            kernel,
            name="exchange_matmul",
            out_shape=(
                jax.ShapeDtypeStruct((row_count, n_dim), jnp.bfloat16),
                jax.ShapeDtypeStruct((CHUNKS, 8, rows, k_dim), jnp.bfloat16),
            ),
            in_specs=[pl.BlockSpec(memory_space=pl.ANY)] * 2,
            out_specs=[pl.BlockSpec(memory_space=pl.ANY)] * 2,
            scratch_shapes=[
                pltpu.VMEM((8 * rows, k_dim), jnp.bfloat16),
                pltpu.VMEM((2, k_dim, COLS), jnp.bfloat16),
                pltpu.VMEM((2, 8 * rows, COLS), f32),
                pltpu.VMEM((2, 4 * rows, COLS), f32),
                pltpu.VMEM((SUMS1, 4 * rows, COLS), f32),
                pltpu.VMEM((SLOTS1, 2 * rows, COLS), f32),
                pltpu.VMEM((SUMS2, 2 * rows, COLS), f32),
                pltpu.VMEM((SLOTS2, rows, COLS), f32),
                pltpu.VMEM((2, rows, COLS), jnp.bfloat16),
                dma((CHUNKS, len(PEERS))),
                dma((CHUNKS, len(PEERS))),
                dma((len(PEERS) + 1,)),
                dma((2,)),
                dma((2,)),
                dma((2,)),
                dma((SUMS1,)),
                dma((SLOTS1,)),
                dma((SUMS2,)),
                dma((SLOTS2,)),
                dma((2,)),
            ],
            compiler_params=pltpu.CompilerParams(
                collective_id=0, has_side_effects=True, vmem_limit_bytes=62 * 1024 * 1024
            ),
            cost_estimate=pl.CostEstimate(
                flops=2 * 8 * row_count * k_dim * n_dim,
                bytes_accessed=2 * CHUNKS * k_dim * n_dim,
                transcendentals=0,
            ),
        )(a_rows, b_rows)
        return c_rows

    return jax.shard_map(
        local_product,
        mesh=mesh,
        in_specs=(P(("mp", "dp"), None), P(("mp", "dp"), None)),
        out_specs=P(("mp", "dp"), None),
        check_vma=False,
    )
```

```python
import functools

import jax
import jax.numpy as jnp
from jax import lax
from jax.experimental import pallas as pl
from jax.experimental.pallas import tpu as pltpu
from jax.sharding import PartitionSpec as P

MESH = pl.DeviceIdType.MESH
PEERS = ((1, 0, 0), (0, 1, 0), (1, 1, 0), (1, 0, 1), (0, 1, 1), (1, 1, 1), (0, 0, 1))
CHUNKS = 8
COLS = 512
PIECE = 2048
AHEAD = 2
HELD = 16
BURST = 2
LAG1 = 5
LAG2 = 4
SUMS1, SUMS2 = HELD + LAG1 + 3, BURST * (LAG2 + 2)
SLOTS1, SLOTS2 = BURST * (2 * LAG1 + 2), BURST * (2 * LAG2 + 2)


def kernel(
    a_ref, b_ref, c_ref, g_ref,
    a_v, b_v, p_v, rd_v, s1_v, r1_v, s2_v, r2_v,
    a_send, a_recv, a_load, b_load, d_send, d_recv, s1_send, r1_recv, s2_send, r2_recv,
):
    _, _, rows, k_dim = g_ref.shape
    half = 4 * rows
    blocks = b_ref.shape[1] // COLS
    pieces = k_dim // PIECE
    steps = CHUNKS * blocks

    y = lax.axis_index("mp")
    x = lax.axis_index("dp") // 2
    c = lax.axis_index("dp") % 2
    f = (1 - c) * x + c * y
    g = (1 - c) * y + c * x
    first = ((1 - c) * y + c * (1 - y), ((1 - c) * (1 - x) + c * x) * 2 + c)
    second = ((1 - c) * (1 - y) + c * y, ((1 - c) * x + c * (1 - x)) * 2 + c)
    sibling = (y, x * 2 + 1 - c)
    me = (y * 2 + x) * 2 + c
    my_pos = 4 * c + 2 * f + g

    def peer(i):
        dx, dy, dc = PEERS[i]
        px, py, pc = (x + dx) % 2, (y + dy) % 2, (c + dc) % 2
        pos = 4 * pc + (1 - pc) * (2 * px + py) + pc * (2 * py + px)
        return (py, px * 2 + pc), (py * 2 + px) * 2 + pc, pos

    def a_rows(j):
        return pl.ds(pl.multiple_of(j * rows, rows), rows)

    def a_copy(i, j, start, size):
        device, index, _ = peer(i)
        return pltpu.make_async_remote_copy(
            src_ref=a_ref.at[a_rows(j), pl.ds(pl.multiple_of(index * k_dim + start, 128), size)],
            dst_ref=g_ref.at[j, my_pos, :, pl.ds(pl.multiple_of(start, 128), size)],
            send_sem=a_send.at[j, i],
            recv_sem=a_recv.at[j, i],
            device_id=device,
            device_id_type=MESH,
        )

    def send_piece(u):
        for i in range(len(PEERS)):
            a_copy(i, u // pieces, (u % pieces) * PIECE, PIECE).start()

    def a_loads(j):
        copies = []
        for i in range(len(PEERS)):
            _, _, pos = peer(i)
            copies.append(pltpu.make_async_copy(
                g_ref.at[j, pos], a_v.at[pl.ds(pl.multiple_of(pos * rows, rows), rows), :], a_load.at[i]
            ))
        copies.append(pltpu.make_async_copy(
            a_ref.at[a_rows(j), pl.ds(pl.multiple_of(me * k_dim, 128), k_dim)],
            a_v.at[pl.ds(pl.multiple_of(my_pos * rows, rows), rows), :],
            a_load.at[len(PEERS)],
        ))
        return copies

    def b_copy(s):
        return pltpu.make_async_copy(
            b_ref.at[:, pl.ds(pl.multiple_of((s % blocks) * COLS, COLS), COLS)], b_v.at[s % 2], b_load.at[s % 2]
        )

    def d_copy(b):
        return pltpu.make_async_remote_copy(
            src_ref=p_v.at[b % 2, pl.ds(pl.multiple_of((1 - c) * half, half), half), :],
            dst_ref=rd_v.at[b % 2],
            send_sem=d_send.at[b % 2],
            recv_sem=d_recv.at[b % 2],
            device_id=sibling,
            device_id_type=MESH,
        )

    def first_copy(b):
        return pltpu.make_async_remote_copy(
            src_ref=s1_v.at[b % SUMS1, pl.ds(pl.multiple_of((1 - f) * 2 * rows, 2 * rows), 2 * rows), :],
            dst_ref=r1_v.at[b % SLOTS1],
            send_sem=s1_send.at[b % SUMS1],
            recv_sem=r1_recv.at[b % SLOTS1],
            device_id=first,
            device_id_type=MESH,
        )

    def second_copy(b):
        return pltpu.make_async_remote_copy(
            src_ref=s2_v.at[b % SUMS2, pl.ds(pl.multiple_of((1 - g) * rows, rows), rows), :],
            dst_ref=r2_v.at[b % SLOTS2],
            send_sem=s2_send.at[b % SUMS2],
            recv_sem=r2_recv.at[b % SLOTS2],
            device_id=second,
            device_id_type=MESH,
        )

    def valid(b):
        return jnp.logical_and(b >= 0, b < steps)

    catch_up = steps - HELD

    def sent(s):
        extra = jnp.maximum(s - catch_up + 1, 0) * (BURST - 1)
        return jnp.clip(jnp.minimum(s - 1, s - 1 - HELD + extra), 0, steps)

    def each(low, high, body):
        for i in range(BURST):
            pl.when(low + i < high)(functools.partial(body, low + i))

    b_copy(0).start()
    barrier = pltpu.get_barrier_semaphore()
    for i in range(len(PEERS)):
        pl.semaphore_signal(barrier, inc=1, device_id=peer(i)[0], device_id_type=MESH)
    pl.semaphore_wait(barrier, len(PEERS))

    @pl.loop(0, pieces + AHEAD)
    def _(u):
        send_piece(u)

    @pl.loop(0, steps + 3 + LAG1 + LAG2)
    def _(s):
        j, n = s // blocks, s % blocks

        @pl.when(s + 1 < steps)
        def _():
            b_copy(s + 1).start()

        @pl.when(valid(s - 1))
        def _():
            d_copy(s - 1).start()

        each(sent(s - 1), sent(s), lambda b: first_copy(b).start())
        each(sent(s - 2 - LAG1), sent(s - 1 - LAG1), lambda b: second_copy(b).start())

        unit = (j + 1) * pieces + n // 2 + AHEAD

        @pl.when(jnp.logical_and(n % 2 == 0, unit < CHUNKS * pieces))
        def _():
            send_piece(unit)

        @pl.when(s < steps)
        def _():
            @pl.when(n == 0)
            def _():
                for i in range(len(PEERS)):
                    a_copy(i, j, 0, k_dim).wait_recv()
                loads = a_loads(j)
                for load in loads:
                    load.start()
                for load in loads:
                    load.wait()

            b_copy(s).wait()

            p_v[s % 2] = jnp.dot(a_v[...], b_v[s % 2], preferred_element_type=jnp.float32)

        @pl.when(valid(s - 1))
        def _():
            b = s - 1
            d_copy(b).wait_recv()
            s1_v[b % SUMS1] = p_v[b % 2, pl.ds(pl.multiple_of(c * half, half), half), :] + rd_v[b % 2]
            d_copy(b).wait_send()

        def add_first(b):
            first_copy(b).wait_recv()
            kept = s1_v[b % SUMS1, pl.ds(pl.multiple_of(f * 2 * rows, 2 * rows), 2 * rows), :]
            s2_v[b % SUMS2] = kept + r1_v[b % SLOTS1]
            first_copy(b).wait_send()

        def add_second(b):
            second_copy(b).wait_recv()
            kept = s2_v[b % SUMS2, pl.ds(pl.multiple_of(g * rows, rows), rows), :]
            part = pl.ds(pl.multiple_of((b % blocks) * COLS, COLS), COLS)
            c_ref[a_rows(b // blocks), part] = (kept + r2_v[b % SLOTS2]).astype(c_ref.dtype)
            second_copy(b).wait_send()

        each(sent(s - 1 - LAG1), sent(s - LAG1), add_first)
        each(sent(s - 2 - LAG1 - LAG2), sent(s - 1 - LAG1 - LAG2), add_second)

    @pl.loop(0, CHUNKS)
    def _(j):
        for i in range(len(PEERS)):
            a_copy(i, j, 0, k_dim).wait_send()


def solution(mesh):
    def local_product(a_rows, b_rows):
        row_count = a_rows.shape[0]
        k_dim, n_dim = b_rows.shape
        rows = row_count // CHUNKS
        f32, dma = jnp.float32, pltpu.SemaphoreType.DMA
        c_rows, _ = pl.pallas_call(
            kernel,
            name="exchange_matmul",
            out_shape=(
                pltpu.VMEM((row_count, n_dim), jnp.bfloat16),
                jax.ShapeDtypeStruct((CHUNKS, 8, rows, k_dim), jnp.bfloat16),
            ),
            in_specs=[pl.BlockSpec(memory_space=pl.ANY)] * 2,
            out_specs=[pl.BlockSpec(memory_space=pltpu.VMEM), pl.BlockSpec(memory_space=pl.ANY)],
            scratch_shapes=[
                pltpu.VMEM((8 * rows, k_dim), jnp.bfloat16),
                pltpu.VMEM((2, k_dim, COLS), jnp.bfloat16),
                pltpu.VMEM((2, 8 * rows, COLS), f32),
                pltpu.VMEM((2, 4 * rows, COLS), f32),
                pltpu.VMEM((SUMS1, 4 * rows, COLS), f32),
                pltpu.VMEM((SLOTS1, 2 * rows, COLS), f32),
                pltpu.VMEM((SUMS2, 2 * rows, COLS), f32),
                pltpu.VMEM((SLOTS2, rows, COLS), f32),
                dma((CHUNKS, len(PEERS))),
                dma((CHUNKS, len(PEERS))),
                dma((len(PEERS) + 1,)),
                dma((2,)),
                dma((2,)),
                dma((2,)),
                dma((SUMS1,)),
                dma((SLOTS1,)),
                dma((SUMS2,)),
                dma((SLOTS2,)),
            ],
            compiler_params=pltpu.CompilerParams(
                collective_id=0, has_side_effects=True, vmem_limit_bytes=56 * 1024 * 1024
            ),
            cost_estimate=pl.CostEstimate(
                flops=2 * 8 * row_count * k_dim * n_dim,
                bytes_accessed=2 * CHUNKS * k_dim * n_dim,
                transcendentals=0,
            ),
        )(a_rows, b_rows)
        return c_rows

    return jax.shard_map(
        local_product,
        mesh=mesh,
        in_specs=(P(("mp", "dp"), None), P(("mp", "dp"), None)),
        out_specs=P(("mp", "dp"), None),
        check_vma=False,
    )
```

```python
import functools

import jax
import jax.numpy as jnp
from jax import lax
from jax.experimental import pallas as pl
from jax.experimental.pallas import tpu as pltpu
from jax.sharding import PartitionSpec as P

MESH = pl.DeviceIdType.MESH
PEERS = ((1, 0, 0), (0, 1, 0), (1, 1, 0), (1, 0, 1), (0, 1, 1), (1, 1, 1), (0, 0, 1))
CHUNKS = 8
COLS = 512
PIECE = 2048
AHEAD = 2
HELD = 12
BURST = 2
LAG1 = 4
LAG2 = 3
SUMS1, SUMS2 = HELD + LAG1 + 3, BURST * (LAG2 + 2)
SLOTS1, SLOTS2 = BURST * (2 * LAG1 + 2), BURST * (2 * LAG2 + 2)
SENDS1, SENDS2 = BURST * (LAG1 + 1), BURST * (LAG2 + 1)
ARRIVING = 3
BUFFERS = 3


def kernel(
    a_ref, b_ref, c_ref, g_ref,
    first_v, a_v, b_v, p_v, rd_v, s1_v, r1_v, s2_v, r2_v,
    first_load, a_send, a_recv, a_load, b_load, d_send, d_recv, s1_send, r1_recv, s2_send, r2_recv,
):
    _, all_rows, k_dim = g_ref.shape
    rows = all_rows // CHUNKS
    half = 4 * rows
    blocks = b_ref.shape[1] // COLS
    pieces = k_dim // PIECE
    steps = CHUNKS * blocks

    y = lax.axis_index("mp")
    x = lax.axis_index("dp") // 2
    c = lax.axis_index("dp") % 2
    f = (1 - c) * x + c * y
    g = (1 - c) * y + c * x
    first = ((1 - c) * y + c * (1 - y), ((1 - c) * (1 - x) + c * x) * 2 + c)
    second = ((1 - c) * (1 - y) + c * y, ((1 - c) * x + c * (1 - x)) * 2 + c)
    sibling = (y, x * 2 + 1 - c)
    me = (y * 2 + x) * 2 + c
    my_pos = 4 * c + 2 * f + g

    def peer(i):
        dx, dy, dc = PEERS[i]
        px, py, pc = (x + dx) % 2, (y + dy) % 2, (c + dc) % 2
        pos = 4 * pc + (1 - pc) * (2 * px + py) + pc * (2 * py + px)
        return (py, px * 2 + pc), (py * 2 + px) * 2 + pc, pos

    def a_rows(j):
        return pl.ds(pl.multiple_of(j * rows, rows), rows)

    def a_columns(i, start, size):
        return pl.ds(pl.multiple_of(peer(i)[1] * k_dim + start, 128), size)

    def a_copy(i, j, start, size, src_ref=None):
        return pltpu.make_async_remote_copy(
            src_ref=a_ref.at[a_rows(j), a_columns(i, start, size)] if src_ref is None else src_ref,
            dst_ref=g_ref.at[my_pos, a_rows(j), pl.ds(pl.multiple_of(start, 128), size)],
            send_sem=a_send.at[i],
            recv_sem=a_recv.at[j % ARRIVING, i],
            device_id=peer(i)[0],
            device_id_type=MESH,
        )

    def a_sent(i):
        return pltpu.make_async_remote_copy(
            src_ref=a_ref.at[:, a_columns(i, 0, k_dim)],
            dst_ref=g_ref.at[my_pos],
            send_sem=a_send.at[i],
            recv_sem=a_recv.at[0, i],
            device_id=peer(i)[0],
            device_id_type=MESH,
        )

    def first_piece(i):
        return pltpu.make_async_copy(a_ref.at[a_rows(0), a_columns(i, 0, PIECE)], first_v.at[i], first_load.at[i])

    def send_piece(u):
        for i in range(len(PEERS)):
            a_copy(i, u // pieces, (u % pieces) * PIECE, PIECE).start()

    def a_loads(j):
        copies = []
        for i in range(len(PEERS)):
            _, _, pos = peer(i)
            copies.append(pltpu.make_async_copy(
                g_ref.at[pos, a_rows(j)], a_v.at[pl.ds(pl.multiple_of(pos * rows, rows), rows), :], a_load.at[i]
            ))
        copies.append(pltpu.make_async_copy(
            a_ref.at[a_rows(j), pl.ds(pl.multiple_of(me * k_dim, 128), k_dim)],
            a_v.at[pl.ds(pl.multiple_of(my_pos * rows, rows), rows), :],
            a_load.at[len(PEERS)],
        ))
        return copies

    def b_copy(s):
        return pltpu.make_async_copy(
            b_ref.at[:, pl.ds(pl.multiple_of((s % blocks) * COLS, COLS), COLS)], b_v.at[s % BUFFERS], b_load.at[s % BUFFERS]
        )

    def d_copy(b):
        return pltpu.make_async_remote_copy(
            src_ref=p_v.at[b % 2, pl.ds(pl.multiple_of((1 - c) * half, half), half), :],
            dst_ref=rd_v.at[b % 2],
            send_sem=d_send.at[b % 2],
            recv_sem=d_recv.at[b % 2],
            device_id=sibling,
            device_id_type=MESH,
        )

    def first_copy(b):
        return pltpu.make_async_remote_copy(
            src_ref=s1_v.at[b % SUMS1, pl.ds(pl.multiple_of((1 - f) * 2 * rows, 2 * rows), 2 * rows), :],
            dst_ref=r1_v.at[b % SLOTS1],
            send_sem=s1_send.at[b % SENDS1],
            recv_sem=r1_recv.at[b % SLOTS1],
            device_id=first,
            device_id_type=MESH,
        )

    def second_copy(b):
        return pltpu.make_async_remote_copy(
            src_ref=s2_v.at[b % SUMS2, pl.ds(pl.multiple_of((1 - g) * rows, rows), rows), :],
            dst_ref=r2_v.at[b % SLOTS2],
            send_sem=s2_send.at[b % SENDS2],
            recv_sem=r2_recv.at[b % SLOTS2],
            device_id=second,
            device_id_type=MESH,
        )

    def valid(b):
        return jnp.logical_and(b >= 0, b < steps)

    catch_up = steps - HELD

    def sent(s):
        extra = jnp.maximum(s - catch_up + 1, 0) * (BURST - 1)
        return jnp.clip(jnp.minimum(s - 1, s - 1 - HELD + extra), 0, steps)

    def each(low, high, body):
        for i in range(BURST):
            pl.when(low + i < high)(functools.partial(body, low + i))

    barrier = pltpu.get_barrier_semaphore()
    for i in range(len(PEERS)):
        pl.semaphore_signal(barrier, inc=1, device_id=peer(i)[0], device_id_type=MESH)
    for i in range(len(PEERS)):
        first_piece(i).start()
    for s in range(BUFFERS - 1):
        b_copy(s).start()
    pl.semaphore_wait(barrier, len(PEERS))

    for i in range(len(PEERS)):
        first_piece(i).wait()
        a_copy(i, 0, 0, PIECE, first_v.at[i]).start()

    @pl.loop(1, pieces + AHEAD)
    def _(u):
        send_piece(u)

    @pl.loop(0, steps + 3 + LAG1 + LAG2)
    def _(s):
        j, n = s // blocks, s % blocks

        @pl.when(s + BUFFERS - 1 < steps)
        def _():
            b_copy(s + BUFFERS - 1).start()

        @pl.when(valid(s - 1))
        def _():
            d_copy(s - 1).start()

        each(sent(s - 1), sent(s), lambda b: first_copy(b).start())
        each(sent(s - 2 - LAG1), sent(s - 1 - LAG1), lambda b: second_copy(b).start())

        unit = (j + 1) * pieces + n // 2 + AHEAD

        @pl.when(jnp.logical_and(n % 2 == 0, unit < CHUNKS * pieces))
        def _():
            send_piece(unit)

        @pl.when(s < steps)
        def _():
            @pl.when(n == 0)
            def _():
                for i in range(len(PEERS)):
                    a_copy(i, j, 0, k_dim).wait_recv()
                loads = a_loads(j)
                for load in loads:
                    load.start()
                for load in loads:
                    load.wait()

            b_copy(s).wait()

            p_v[s % 2] = jnp.dot(a_v[...], b_v[s % BUFFERS], preferred_element_type=jnp.float32)

        @pl.when(valid(s - 1))
        def _():
            b = s - 1
            d_copy(b).wait_recv()
            s1_v[b % SUMS1] = p_v[b % 2, pl.ds(pl.multiple_of(c * half, half), half), :] + rd_v[b % 2]
            d_copy(b).wait_send()

        def add_first(b):
            first_copy(b).wait_recv()
            kept = s1_v[b % SUMS1, pl.ds(pl.multiple_of(f * 2 * rows, 2 * rows), 2 * rows), :]
            s2_v[b % SUMS2] = kept + r1_v[b % SLOTS1]
            first_copy(b).wait_send()

        def add_second(b):
            second_copy(b).wait_recv()
            kept = s2_v[b % SUMS2, pl.ds(pl.multiple_of(g * rows, rows), rows), :]
            part = pl.ds(pl.multiple_of((b % blocks) * COLS, COLS), COLS)
            c_ref[a_rows(b // blocks), part] = (kept + r2_v[b % SLOTS2]).astype(c_ref.dtype)
            second_copy(b).wait_send()

        each(sent(s - 1 - LAG1), sent(s - LAG1), add_first)
        each(sent(s - 2 - LAG1 - LAG2), sent(s - 1 - LAG1 - LAG2), add_second)

    for i in range(len(PEERS)):
        a_sent(i).wait_send()


def solution(mesh):
    def local_product(a_rows, b_rows):
        row_count = a_rows.shape[0]
        k_dim, n_dim = b_rows.shape
        rows = row_count // CHUNKS
        f32, dma = jnp.float32, pltpu.SemaphoreType.DMA
        c_rows, _ = pl.pallas_call(
            kernel,
            name="exchange_matmul",
            out_shape=(
                pltpu.VMEM((row_count, n_dim), jnp.bfloat16),
                jax.ShapeDtypeStruct((8, row_count, k_dim), jnp.bfloat16),
            ),
            in_specs=[pl.BlockSpec(memory_space=pl.ANY)] * 2,
            out_specs=[pl.BlockSpec(memory_space=pltpu.VMEM), pl.BlockSpec(memory_space=pl.ANY)],
            scratch_shapes=[
                pltpu.VMEM((len(PEERS), rows, PIECE), jnp.bfloat16),
                pltpu.VMEM((8 * rows, k_dim), jnp.bfloat16),
                pltpu.VMEM((BUFFERS, k_dim, COLS), jnp.bfloat16),
                pltpu.VMEM((2, 8 * rows, COLS), f32),
                pltpu.VMEM((2, 4 * rows, COLS), f32),
                pltpu.VMEM((SUMS1, 4 * rows, COLS), f32),
                pltpu.VMEM((SLOTS1, 2 * rows, COLS), f32),
                pltpu.VMEM((SUMS2, 2 * rows, COLS), f32),
                pltpu.VMEM((SLOTS2, rows, COLS), f32),
                dma((len(PEERS),)),
                dma((len(PEERS),)),
                dma((ARRIVING, len(PEERS))),
                dma((len(PEERS) + 1,)),
                dma((BUFFERS,)),
                dma((2,)),
                dma((2,)),
                dma((SENDS1,)),
                dma((SLOTS1,)),
                dma((SENDS2,)),
                dma((SLOTS2,)),
            ],
            compiler_params=pltpu.CompilerParams(
                collective_id=0, has_side_effects=True, vmem_limit_bytes=59 * 1024 * 1024
            ),
            cost_estimate=pl.CostEstimate(
                flops=2 * 8 * row_count * k_dim * n_dim,
                bytes_accessed=2 * CHUNKS * k_dim * n_dim,
                transcendentals=0,
            ),
        )(a_rows, b_rows)
        return c_rows

    return jax.shard_map(
        local_product,
        mesh=mesh,
        in_specs=(P(("mp", "dp"), None), P(("mp", "dp"), None)),
        out_specs=P(("mp", "dp"), None),
        check_vma=False,
    )
```

```python
import functools

import jax
import jax.numpy as jnp
from jax import lax
from jax.experimental import pallas as pl
from jax.experimental.pallas import tpu as pltpu
from jax.sharding import PartitionSpec as P

MESH = pl.DeviceIdType.MESH
PEERS = ((1, 0, 0), (0, 1, 0), (1, 1, 0), (1, 0, 1), (0, 1, 1), (1, 1, 1), (0, 0, 1))
CHUNKS = 8
COLS = 512
PIECE = 2048
AHEAD = 2
HELD = 12
BURST = 2
LAG1 = 4
LAG2 = 3
HELD2 = 4
SUMS1, SUMS2 = HELD + LAG1 + 3, BURST * (HELD2 + LAG2 + 2)
SLOTS1, SLOTS2 = BURST * (2 * LAG1 + 2), BURST * (2 * LAG2 + 2)
SENDS1, SENDS2 = BURST * (LAG1 + 1), BURST * (LAG2 + 1)
ARRIVING = 3
BUFFERS = 3


def kernel(
    a_ref, b_ref, c_ref, g_ref,
    first_v, a_v, b_v, p_v, rd_v, s1_v, r1_v, s2_v, r2_v,
    a_send, a_recv, a_load, b_load, d_send, d_recv, s1_send, r1_recv, s2_send, r2_recv,
):
    _, all_rows, k_dim = g_ref.shape
    rows = all_rows // CHUNKS
    half = 4 * rows
    blocks = b_ref.shape[1] // COLS
    pieces = k_dim // PIECE
    steps = CHUNKS * blocks

    y = lax.axis_index("mp")
    x = lax.axis_index("dp") // 2
    c = lax.axis_index("dp") % 2
    f = (1 - c) * x + c * y
    g = (1 - c) * y + c * x
    first = ((1 - c) * y + c * (1 - y), ((1 - c) * (1 - x) + c * x) * 2 + c)
    second = ((1 - c) * (1 - y) + c * y, ((1 - c) * x + c * (1 - x)) * 2 + c)
    sibling = (y, x * 2 + 1 - c)
    me = (y * 2 + x) * 2 + c
    my_pos = 4 * c + 2 * f + g

    def peer(i):
        dx, dy, dc = PEERS[i]
        px, py, pc = (x + dx) % 2, (y + dy) % 2, (c + dc) % 2
        pos = 4 * pc + (1 - pc) * (2 * px + py) + pc * (2 * py + px)
        return (py, px * 2 + pc), (py * 2 + px) * 2 + pc, pos

    def a_rows(j):
        return pl.ds(pl.multiple_of(j * rows, rows), rows)

    def a_columns(i, start, size):
        return pl.ds(pl.multiple_of(peer(i)[1] * k_dim + start, 128), size)

    def a_copy(i, j, start, size, src_ref=None):
        return pltpu.make_async_remote_copy(
            src_ref=a_ref.at[a_rows(j), a_columns(i, start, size)] if src_ref is None else src_ref,
            dst_ref=g_ref.at[my_pos, a_rows(j), pl.ds(pl.multiple_of(start, 128), size)],
            send_sem=a_send.at[i],
            recv_sem=a_recv.at[j % ARRIVING, i],
            device_id=peer(i)[0],
            device_id_type=MESH,
        )

    def a_sent(i):
        return pltpu.make_async_remote_copy(
            src_ref=a_ref.at[:, a_columns(i, 0, k_dim)],
            dst_ref=g_ref.at[my_pos],
            send_sem=a_send.at[i],
            recv_sem=a_recv.at[0, i],
            device_id=peer(i)[0],
            device_id_type=MESH,
        )

    def first_piece(i):
        return pltpu.make_async_copy(a_ref.at[a_rows(0), a_columns(i, 0, PIECE)], first_v.at[i], a_load.at[i])

    def send_piece(u):
        for i in range(len(PEERS)):
            a_copy(i, u // pieces, (u % pieces) * PIECE, PIECE).start()

    def a_loads(j):
        copies = []
        for i in range(len(PEERS)):
            _, _, pos = peer(i)
            copies.append(pltpu.make_async_copy(
                g_ref.at[pos, a_rows(j)], a_v.at[pl.ds(pl.multiple_of(pos * rows, rows), rows), :], a_load.at[i]
            ))
        copies.append(pltpu.make_async_copy(
            a_ref.at[a_rows(j), pl.ds(pl.multiple_of(me * k_dim, 128), k_dim)],
            a_v.at[pl.ds(pl.multiple_of(my_pos * rows, rows), rows), :],
            a_load.at[len(PEERS)],
        ))
        return copies

    def b_copy(s):
        return pltpu.make_async_copy(
            b_ref.at[:, pl.ds(pl.multiple_of((s % blocks) * COLS, COLS), COLS)], b_v.at[s % BUFFERS], b_load.at[s % BUFFERS]
        )

    def d_copy(b):
        return pltpu.make_async_remote_copy(
            src_ref=p_v.at[b % 2, pl.ds(pl.multiple_of((1 - c) * half, half), half), :],
            dst_ref=rd_v.at[b % 2],
            send_sem=d_send.at[b % 2],
            recv_sem=d_recv.at[b % 2],
            device_id=sibling,
            device_id_type=MESH,
        )

    def first_copy(b):
        return pltpu.make_async_remote_copy(
            src_ref=s1_v.at[b % SUMS1, pl.ds(pl.multiple_of((1 - f) * 2 * rows, 2 * rows), 2 * rows), :],
            dst_ref=r1_v.at[b % SLOTS1],
            send_sem=s1_send.at[b % SENDS1],
            recv_sem=r1_recv.at[b % SLOTS1],
            device_id=first,
            device_id_type=MESH,
        )

    def second_copy(b):
        return pltpu.make_async_remote_copy(
            src_ref=s2_v.at[b % SUMS2, pl.ds(pl.multiple_of((1 - g) * rows, rows), rows), :],
            dst_ref=r2_v.at[b % SLOTS2],
            send_sem=s2_send.at[b % SENDS2],
            recv_sem=r2_recv.at[b % SLOTS2],
            device_id=second,
            device_id_type=MESH,
        )

    def valid(b):
        return jnp.logical_and(b >= 0, b < steps)

    catch_up = steps - HELD

    def sent(s):
        extra = jnp.maximum(s - catch_up + 1, 0) * (BURST - 1)
        return jnp.clip(jnp.minimum(s - 1, s - 1 - HELD + extra), 0, steps)

    def each(low, high, body):
        for i in range(BURST):
            pl.when(low + i < high)(functools.partial(body, low + i))

    barrier = pltpu.get_barrier_semaphore()
    for i in range(len(PEERS)):
        pl.semaphore_signal(barrier, inc=1, device_id=peer(i)[0], device_id_type=MESH)
    for i in range(len(PEERS)):
        first_piece(i).start()
    for s in range(BUFFERS - 1):
        b_copy(s).start()
    pl.semaphore_wait(barrier, len(PEERS))

    for i in range(len(PEERS)):
        first_piece(i).wait()
        a_copy(i, 0, 0, PIECE, first_v.at[i]).start()

    @pl.loop(1, pieces + AHEAD)
    def _(u):
        send_piece(u)

    @pl.loop(0, steps + 3 + LAG1 + HELD2 + LAG2)
    def _(s):
        j, n = s // blocks, s % blocks

        @pl.when(s + BUFFERS - 1 < steps)
        def _():
            b_copy(s + BUFFERS - 1).start()

        @pl.when(valid(s - 1))
        def _():
            d_copy(s - 1).start()

        each(sent(s - 1), sent(s), lambda b: first_copy(b).start())
        each(sent(s - 2 - LAG1 - HELD2), sent(s - 1 - LAG1 - HELD2), lambda b: second_copy(b).start())

        unit = (j + 1) * pieces + n // 2 + AHEAD

        @pl.when(jnp.logical_and(n % 2 == 0, unit < CHUNKS * pieces))
        def _():
            send_piece(unit)

        @pl.when(s < steps)
        def _():
            @pl.when(n == 0)
            def _():
                for i in range(len(PEERS)):
                    a_copy(i, j, 0, k_dim).wait_recv()
                loads = a_loads(j)
                for load in loads:
                    load.start()
                for load in loads:
                    load.wait()

            b_copy(s).wait()

            p_v[s % 2] = jnp.dot(a_v[...], b_v[s % BUFFERS], preferred_element_type=jnp.float32)

        @pl.when(valid(s - 1))
        def _():
            b = s - 1
            d_copy(b).wait_recv()
            s1_v[b % SUMS1] = p_v[b % 2, pl.ds(pl.multiple_of(c * half, half), half), :] + rd_v[b % 2]
            d_copy(b).wait_send()

        def add_first(b):
            first_copy(b).wait_recv()
            kept = s1_v[b % SUMS1, pl.ds(pl.multiple_of(f * 2 * rows, 2 * rows), 2 * rows), :]
            s2_v[b % SUMS2] = kept + r1_v[b % SLOTS1]
            first_copy(b).wait_send()

        def add_second(b):
            second_copy(b).wait_recv()
            kept = s2_v[b % SUMS2, pl.ds(pl.multiple_of(g * rows, rows), rows), :]
            part = pl.ds(pl.multiple_of((b % blocks) * COLS, COLS), COLS)
            c_ref[a_rows(b // blocks), part] = (kept + r2_v[b % SLOTS2]).astype(c_ref.dtype)
            second_copy(b).wait_send()

        each(sent(s - 1 - LAG1), sent(s - LAG1), add_first)
        each(sent(s - 2 - LAG1 - HELD2 - LAG2), sent(s - 1 - LAG1 - HELD2 - LAG2), add_second)

    for i in range(len(PEERS)):
        a_sent(i).wait_send()


def solution(mesh):
    def local_product(a_rows, b_rows):
        row_count = a_rows.shape[0]
        k_dim, n_dim = b_rows.shape
        rows = row_count // CHUNKS
        f32, dma = jnp.float32, pltpu.SemaphoreType.DMA
        c_rows, _ = pl.pallas_call(
            kernel,
            name="exchange_matmul",
            out_shape=(
                pltpu.VMEM((row_count, n_dim), jnp.bfloat16),
                jax.ShapeDtypeStruct((8, row_count, k_dim), jnp.bfloat16),
            ),
            in_specs=[pl.BlockSpec(memory_space=pl.ANY)] * 2,
            out_specs=[pl.BlockSpec(memory_space=pltpu.VMEM), pl.BlockSpec(memory_space=pl.ANY)],
            scratch_shapes=[
                pltpu.VMEM((len(PEERS), rows, PIECE), jnp.bfloat16),
                pltpu.VMEM((8 * rows, k_dim), jnp.bfloat16),
                pltpu.VMEM((BUFFERS, k_dim, COLS), jnp.bfloat16),
                pltpu.VMEM((2, 8 * rows, COLS), f32),
                pltpu.VMEM((2, 4 * rows, COLS), f32),
                pltpu.VMEM((SUMS1, 4 * rows, COLS), f32),
                pltpu.VMEM((SLOTS1, 2 * rows, COLS), f32),
                pltpu.VMEM((SUMS2, 2 * rows, COLS), f32),
                pltpu.VMEM((SLOTS2, rows, COLS), f32),
                dma((len(PEERS),)),
                dma((ARRIVING, len(PEERS))),
                dma((len(PEERS) + 1,)),
                dma((BUFFERS,)),
                dma((2,)),
                dma((2,)),
                dma((SENDS1,)),
                dma((SLOTS1,)),
                dma((SENDS2,)),
                dma((SLOTS2,)),
            ],
            compiler_params=pltpu.CompilerParams(
                collective_id=0, has_side_effects=True, vmem_limit_bytes=59 * 1024 * 1024
            ),
            cost_estimate=pl.CostEstimate(
                flops=2 * 8 * row_count * k_dim * n_dim,
                bytes_accessed=2 * CHUNKS * k_dim * n_dim,
                transcendentals=0,
            ),
        )(a_rows, b_rows)
        return c_rows

    return jax.shard_map(
        local_product,
        mesh=mesh,
        in_specs=(P(("mp", "dp"), None), P(("mp", "dp"), None)),
        out_specs=P(("mp", "dp"), None),
        check_vma=False,
    )
```

```python
import functools

import jax
import jax.numpy as jnp
from jax import lax
from jax.experimental import pallas as pl
from jax.experimental.pallas import tpu as pltpu
from jax.sharding import PartitionSpec as P

MESH = pl.DeviceIdType.MESH
PEERS = ((1, 0, 0), (0, 1, 0), (1, 1, 0), (1, 0, 1), (0, 1, 1), (1, 1, 1), (0, 0, 1))
CHUNKS = 8
COLS = 512
PIECE = 2048
AHEAD = 2
HELD = 12
BURST = 2
LAG1 = 4
LAG2 = 3
HELD2 = 4
SUMS1, SUMS2 = HELD + LAG1 + 3, BURST * (HELD2 + LAG2 + 2)
SLOTS1, SLOTS2 = BURST * (2 * LAG1 + 2), BURST * (2 * LAG2 + 2)
SENDS1, SENDS2 = BURST * (LAG1 + 1), BURST * (LAG2 + 1)
ARRIVING = 3
BUFFERS = 3


def kernel(
    a_ref, b_ref, c_ref, g_ref,
    first_v, a_v, b_v, p_v, rd_v, s1_v, r1_v, s2_v, r2_v,
    a_send, a_recv, a_load, b_load, d_send, d_recv, s1_send, r1_recv, s2_send, r2_recv,
):
    _, all_rows, k_dim = g_ref.shape
    rows = all_rows // CHUNKS
    half = 4 * rows
    blocks = b_ref.shape[1] // COLS
    pieces = k_dim // PIECE
    steps = CHUNKS * blocks

    y = lax.axis_index("mp")
    x = lax.axis_index("dp") // 2
    c = lax.axis_index("dp") % 2
    f = (1 - c) * x + c * y
    g = (1 - c) * y + c * x
    first = ((1 - c) * y + c * (1 - y), ((1 - c) * (1 - x) + c * x) * 2 + c)
    second = ((1 - c) * (1 - y) + c * y, ((1 - c) * x + c * (1 - x)) * 2 + c)
    sibling = (y, x * 2 + 1 - c)
    me = (y * 2 + x) * 2 + c
    my_pos = 4 * c + 2 * f + g

    def peer(i):
        dx, dy, dc = PEERS[i]
        px, py, pc = (x + dx) % 2, (y + dy) % 2, (c + dc) % 2
        pos = 4 * pc + (1 - pc) * (2 * px + py) + pc * (2 * py + px)
        return (py, px * 2 + pc), (py * 2 + px) * 2 + pc, pos

    def a_rows(j):
        return pl.ds(pl.multiple_of(j * rows, rows), rows)

    def a_columns(i, start, size):
        return pl.ds(pl.multiple_of(peer(i)[1] * k_dim + start, 128), size)

    def a_copy(i, j, start, size, src_ref=None):
        return pltpu.make_async_remote_copy(
            src_ref=a_ref.at[a_rows(j), a_columns(i, start, size)] if src_ref is None else src_ref,
            dst_ref=g_ref.at[my_pos, a_rows(j), pl.ds(pl.multiple_of(start, 128), size)],
            send_sem=a_send.at[i],
            recv_sem=a_recv.at[j % ARRIVING],
            device_id=peer(i)[0],
            device_id_type=MESH,
        )

    def a_sent(i):
        return pltpu.make_async_remote_copy(
            src_ref=a_ref.at[:, a_columns(i, 0, k_dim)],
            dst_ref=g_ref.at[my_pos],
            send_sem=a_send.at[i],
            recv_sem=a_recv.at[0],
            device_id=peer(i)[0],
            device_id_type=MESH,
        )

    def first_piece(i):
        return pltpu.make_async_copy(a_ref.at[a_rows(0), a_columns(i, 0, PIECE)], first_v.at[i], a_load)

    def send_piece(u):
        for i in range(len(PEERS)):
            a_copy(i, u // pieces, (u % pieces) * PIECE, PIECE).start()

    def a_loads(j):
        copies = []
        for i in range(len(PEERS)):
            _, _, pos = peer(i)
            copies.append(pltpu.make_async_copy(
                g_ref.at[pos, a_rows(j)], a_v.at[pl.ds(pl.multiple_of(pos * rows, rows), rows), :], a_load
            ))
        copies.append(pltpu.make_async_copy(
            a_ref.at[a_rows(j), pl.ds(pl.multiple_of(me * k_dim, 128), k_dim)],
            a_v.at[pl.ds(pl.multiple_of(my_pos * rows, rows), rows), :],
            a_load,
        ))
        return copies

    def b_copy(s):
        return pltpu.make_async_copy(
            b_ref.at[:, pl.ds(pl.multiple_of((s % blocks) * COLS, COLS), COLS)], b_v.at[s % BUFFERS], b_load.at[s % BUFFERS]
        )

    def d_copy(b):
        return pltpu.make_async_remote_copy(
            src_ref=p_v.at[b % 2, pl.ds(pl.multiple_of((1 - c) * half, half), half), :],
            dst_ref=rd_v.at[b % 2],
            send_sem=d_send.at[b % 2],
            recv_sem=d_recv.at[b % 2],
            device_id=sibling,
            device_id_type=MESH,
        )

    def first_copy(b):
        return pltpu.make_async_remote_copy(
            src_ref=s1_v.at[b % SUMS1, pl.ds(pl.multiple_of((1 - f) * 2 * rows, 2 * rows), 2 * rows), :],
            dst_ref=r1_v.at[b % SLOTS1],
            send_sem=s1_send.at[b % SENDS1],
            recv_sem=r1_recv.at[b % SLOTS1],
            device_id=first,
            device_id_type=MESH,
        )

    def second_copy(b):
        return pltpu.make_async_remote_copy(
            src_ref=s2_v.at[b % SUMS2, pl.ds(pl.multiple_of((1 - g) * rows, rows), rows), :],
            dst_ref=r2_v.at[b % SLOTS2],
            send_sem=s2_send.at[b % SENDS2],
            recv_sem=r2_recv.at[b % SLOTS2],
            device_id=second,
            device_id_type=MESH,
        )

    def valid(b):
        return jnp.logical_and(b >= 0, b < steps)

    catch_up = steps - HELD

    def sent(s):
        extra = jnp.maximum(s - catch_up + 1, 0) * (BURST - 1)
        return jnp.clip(jnp.minimum(s - 1, s - 1 - HELD + extra), 0, steps)

    def each(low, high, body):
        for i in range(BURST):
            pl.when(low + i < high)(functools.partial(body, low + i))

    barrier = pltpu.get_barrier_semaphore()
    for i in range(len(PEERS)):
        pl.semaphore_signal(barrier, inc=1, device_id=peer(i)[0], device_id_type=MESH)
    for i in range(len(PEERS)):
        first_piece(i).start()
    for s in range(BUFFERS - 1):
        b_copy(s).start()
    pl.semaphore_wait(barrier, len(PEERS))

    pltpu.make_async_copy(g_ref.at[pl.ds(0, len(PEERS)), a_rows(0), pl.ds(0, PIECE)], first_v, a_load).wait()
    for i in range(len(PEERS)):
        a_copy(i, 0, 0, PIECE, first_v.at[i]).start()

    @pl.loop(1, pieces + AHEAD)
    def _(u):
        send_piece(u)

    @pl.loop(0, steps + 3 + LAG1 + HELD2 + LAG2)
    def _(s):
        j, n = s // blocks, s % blocks

        @pl.when(s + BUFFERS - 1 < steps)
        def _():
            b_copy(s + BUFFERS - 1).start()

        @pl.when(valid(s - 1))
        def _():
            d_copy(s - 1).start()

        each(sent(s - 1), sent(s), lambda b: first_copy(b).start())
        each(sent(s - 2 - LAG1 - HELD2), sent(s - 1 - LAG1 - HELD2), lambda b: second_copy(b).start())

        unit = (j + 1) * pieces + n // 2 + AHEAD

        @pl.when(jnp.logical_and(n % 2 == 0, unit < CHUNKS * pieces))
        def _():
            send_piece(unit)

        @pl.when(s < steps)
        def _():
            @pl.when(n == 0)
            def _():
                arrived = g_ref.at[pl.ds(0, len(PEERS)), a_rows(j)]
                pltpu.make_async_copy(arrived, arrived, a_recv.at[j % ARRIVING]).wait()
                for load in a_loads(j):
                    load.start()
                pltpu.make_async_copy(a_ref.at[:, pl.ds(0, k_dim)], a_v, a_load).wait()

            b_copy(s).wait()

            p_v[s % 2] = jnp.dot(a_v[...], b_v[s % BUFFERS], preferred_element_type=jnp.float32)

        @pl.when(valid(s - 1))
        def _():
            b = s - 1
            d_copy(b).wait_recv()
            s1_v[b % SUMS1] = p_v[b % 2, pl.ds(pl.multiple_of(c * half, half), half), :] + rd_v[b % 2]
            d_copy(b).wait_send()

        def add_first(b):
            first_copy(b).wait_recv()
            kept = s1_v[b % SUMS1, pl.ds(pl.multiple_of(f * 2 * rows, 2 * rows), 2 * rows), :]
            s2_v[b % SUMS2] = kept + r1_v[b % SLOTS1]
            first_copy(b).wait_send()

        def add_second(b):
            second_copy(b).wait_recv()
            kept = s2_v[b % SUMS2, pl.ds(pl.multiple_of(g * rows, rows), rows), :]
            part = pl.ds(pl.multiple_of((b % blocks) * COLS, COLS), COLS)
            c_ref[a_rows(b // blocks), part] = (kept + r2_v[b % SLOTS2]).astype(c_ref.dtype)
            second_copy(b).wait_send()

        each(sent(s - 1 - LAG1), sent(s - LAG1), add_first)
        each(sent(s - 2 - LAG1 - HELD2 - LAG2), sent(s - 1 - LAG1 - HELD2 - LAG2), add_second)

    for i in range(len(PEERS)):
        a_sent(i).wait_send()


def solution(mesh):
    def local_product(a_rows, b_rows):
        row_count = a_rows.shape[0]
        k_dim, n_dim = b_rows.shape
        rows = row_count // CHUNKS
        f32, dma = jnp.float32, pltpu.SemaphoreType.DMA
        c_rows, _ = pl.pallas_call(
            kernel,
            name="exchange_matmul",
            out_shape=(
                pltpu.VMEM((row_count, n_dim), jnp.bfloat16),
                jax.ShapeDtypeStruct((8, row_count, k_dim), jnp.bfloat16),
            ),
            in_specs=[pl.BlockSpec(memory_space=pl.ANY)] * 2,
            out_specs=[pl.BlockSpec(memory_space=pltpu.VMEM), pl.BlockSpec(memory_space=pl.ANY)],
            scratch_shapes=[
                pltpu.VMEM((len(PEERS), rows, PIECE), jnp.bfloat16),
                pltpu.VMEM((8 * rows, k_dim), jnp.bfloat16),
                pltpu.VMEM((BUFFERS, k_dim, COLS), jnp.bfloat16),
                pltpu.VMEM((2, 8 * rows, COLS), f32),
                pltpu.VMEM((2, 4 * rows, COLS), f32),
                pltpu.VMEM((SUMS1, 4 * rows, COLS), f32),
                pltpu.VMEM((SLOTS1, 2 * rows, COLS), f32),
                pltpu.VMEM((SUMS2, 2 * rows, COLS), f32),
                pltpu.VMEM((SLOTS2, rows, COLS), f32),
                dma((len(PEERS),)),
                dma((ARRIVING,)),
                dma(()),
                dma((BUFFERS,)),
                dma((2,)),
                dma((2,)),
                dma((SENDS1,)),
                dma((SLOTS1,)),
                dma((SENDS2,)),
                dma((SLOTS2,)),
            ],
            compiler_params=pltpu.CompilerParams(
                collective_id=0, has_side_effects=True, vmem_limit_bytes=59 * 1024 * 1024
            ),
            cost_estimate=pl.CostEstimate(
                flops=2 * 8 * row_count * k_dim * n_dim,
                bytes_accessed=2 * CHUNKS * k_dim * n_dim,
                transcendentals=0,
            ),
        )(a_rows, b_rows)
        return c_rows

    return jax.shard_map(
        local_product,
        mesh=mesh,
        in_specs=(P(("mp", "dp"), None), P(("mp", "dp"), None)),
        out_specs=P(("mp", "dp"), None),
        check_vma=False,
    )
```

```python
import functools

import jax
import jax.numpy as jnp
from jax import lax
from jax.experimental import pallas as pl
from jax.experimental.pallas import tpu as pltpu
from jax.sharding import PartitionSpec as P

MESH = pl.DeviceIdType.MESH
PEERS = ((1, 0, 0), (0, 1, 0), (1, 1, 0), (1, 0, 1), (0, 1, 1), (1, 1, 1), (0, 0, 1))
CHUNKS = 8
COLS = 512
PIECE = 2048
AHEAD = 2
HELD = 16
BURST = 2
LAG1 = 5
LAG2 = 3
HELD2 = 4
SUMS1, SUMS2 = HELD + LAG1 + 3, BURST * (HELD2 + LAG2 + 2)
SLOTS1, SLOTS2 = BURST * (2 * LAG1 + 2), BURST * (2 * LAG2 + 2)
SENDS1, SENDS2 = BURST * (LAG1 + 1), BURST * (LAG2 + 1)
ARRIVING = 3
BUFFERS = 3


def kernel(
    a_ref, b_ref, c_ref, g_ref,
    first_v, a_v, b_v, p_v, rd_v, s1_v, r1_v, s2_v, r2_v,
    a_send, a_recv, a_load, b_load, d_send, d_recv, s1_send, r1_recv, s2_send, r2_recv,
):
    _, all_rows, k_dim = g_ref.shape
    rows = all_rows // CHUNKS
    half = 4 * rows
    blocks = b_ref.shape[1] // COLS
    pieces = k_dim // PIECE
    steps = CHUNKS * blocks

    y = lax.axis_index("mp")
    x = lax.axis_index("dp") // 2
    c = lax.axis_index("dp") % 2
    f = (1 - c) * x + c * y
    g = (1 - c) * y + c * x
    first = ((1 - c) * y + c * (1 - y), ((1 - c) * (1 - x) + c * x) * 2 + c)
    second = ((1 - c) * (1 - y) + c * y, ((1 - c) * x + c * (1 - x)) * 2 + c)
    sibling = (y, x * 2 + 1 - c)
    me = (y * 2 + x) * 2 + c
    my_pos = 4 * c + 2 * f + g

    def peer(i):
        dx, dy, dc = PEERS[i]
        px, py, pc = (x + dx) % 2, (y + dy) % 2, (c + dc) % 2
        pos = 4 * pc + (1 - pc) * (2 * px + py) + pc * (2 * py + px)
        return (py, px * 2 + pc), (py * 2 + px) * 2 + pc, pos

    def a_rows(j):
        return pl.ds(pl.multiple_of(j * rows, rows), rows)

    def a_columns(i, start, size):
        return pl.ds(pl.multiple_of(peer(i)[1] * k_dim + start, 128), size)

    def a_copy(i, j, start, size, src_ref=None):
        return pltpu.make_async_remote_copy(
            src_ref=a_ref.at[a_rows(j), a_columns(i, start, size)] if src_ref is None else src_ref,
            dst_ref=g_ref.at[my_pos, a_rows(j), pl.ds(pl.multiple_of(start, 128), size)],
            send_sem=a_send.at[i],
            recv_sem=a_recv.at[j % ARRIVING, i],
            device_id=peer(i)[0],
            device_id_type=MESH,
        )

    def a_sent(i):
        return pltpu.make_async_remote_copy(
            src_ref=a_ref.at[:, a_columns(i, 0, k_dim)],
            dst_ref=g_ref.at[my_pos],
            send_sem=a_send.at[i],
            recv_sem=a_recv.at[0, i],
            device_id=peer(i)[0],
            device_id_type=MESH,
        )

    def first_piece(i):
        return pltpu.make_async_copy(a_ref.at[a_rows(0), a_columns(i, 0, PIECE)], first_v.at[i], a_load.at[i])

    def send_piece(u):
        for i in range(len(PEERS)):
            a_copy(i, u // pieces, (u % pieces) * PIECE, PIECE).start()

    def a_loads(j):
        copies = []
        for i in range(len(PEERS)):
            _, _, pos = peer(i)
            copies.append(pltpu.make_async_copy(
                g_ref.at[pos, a_rows(j)], a_v.at[pl.ds(pl.multiple_of(pos * rows, rows), rows), :], a_load.at[i]
            ))
        copies.append(pltpu.make_async_copy(
            a_ref.at[a_rows(j), pl.ds(pl.multiple_of(me * k_dim, 128), k_dim)],
            a_v.at[pl.ds(pl.multiple_of(my_pos * rows, rows), rows), :],
            a_load.at[len(PEERS)],
        ))
        return copies

    def b_copy(s):
        return pltpu.make_async_copy(
            b_ref.at[:, pl.ds(pl.multiple_of((s % blocks) * COLS, COLS), COLS)], b_v.at[s % BUFFERS], b_load.at[s % BUFFERS]
        )

    def d_copy(b):
        return pltpu.make_async_remote_copy(
            src_ref=p_v.at[b % 2, pl.ds(pl.multiple_of((1 - c) * half, half), half), :],
            dst_ref=rd_v.at[b % 2],
            send_sem=d_send.at[b % 2],
            recv_sem=d_recv.at[b % 2],
            device_id=sibling,
            device_id_type=MESH,
        )

    def first_copy(b):
        return pltpu.make_async_remote_copy(
            src_ref=s1_v.at[b % SUMS1, pl.ds(pl.multiple_of((1 - f) * 2 * rows, 2 * rows), 2 * rows), :],
            dst_ref=r1_v.at[b % SLOTS1],
            send_sem=s1_send.at[b % SENDS1],
            recv_sem=r1_recv.at[b % SLOTS1],
            device_id=first,
            device_id_type=MESH,
        )

    def second_copy(b):
        return pltpu.make_async_remote_copy(
            src_ref=s2_v.at[b % SUMS2, pl.ds(pl.multiple_of((1 - g) * rows, rows), rows), :],
            dst_ref=r2_v.at[b % SLOTS2],
            send_sem=s2_send.at[b % SENDS2],
            recv_sem=r2_recv.at[b % SLOTS2],
            device_id=second,
            device_id_type=MESH,
        )

    def valid(b):
        return jnp.logical_and(b >= 0, b < steps)

    catch_up = steps - HELD

    def sent(s):
        extra = jnp.maximum(s - catch_up + 1, 0) * (BURST - 1)
        return jnp.clip(jnp.minimum(s - 1, s - 1 - HELD + extra), 0, steps)

    def each(low, high, body):
        for i in range(BURST):
            pl.when(low + i < high)(functools.partial(body, low + i))

    barrier = pltpu.get_barrier_semaphore()
    for i in range(len(PEERS)):
        pl.semaphore_signal(barrier, inc=1, device_id=peer(i)[0], device_id_type=MESH)
    for i in range(len(PEERS)):
        first_piece(i).start()
    for s in range(BUFFERS - 1):
        b_copy(s).start()
    pl.semaphore_wait(barrier, len(PEERS))

    for i in range(len(PEERS)):
        first_piece(i).wait()
        a_copy(i, 0, 0, PIECE, first_v.at[i]).start()

    @pl.loop(1, pieces + AHEAD)
    def _(u):
        send_piece(u)

    @pl.loop(0, steps + 3 + LAG1 + HELD2 + LAG2)
    def _(s):
        j, n = s // blocks, s % blocks

        @pl.when(s + BUFFERS - 1 < steps)
        def _():
            b_copy(s + BUFFERS - 1).start()

        @pl.when(valid(s - 1))
        def _():
            d_copy(s - 1).start()

        each(sent(s - 1), sent(s), lambda b: first_copy(b).start())
        each(sent(s - 2 - LAG1 - HELD2), sent(s - 1 - LAG1 - HELD2), lambda b: second_copy(b).start())

        unit = (j + 1) * pieces + n // 2 + AHEAD

        @pl.when(jnp.logical_and(n % 2 == 0, unit < CHUNKS * pieces))
        def _():
            send_piece(unit)

        @pl.when(s < steps)
        def _():
            @pl.when(n == 0)
            def _():
                for i in range(len(PEERS)):
                    a_copy(i, j, 0, k_dim).wait_recv()
                loads = a_loads(j)
                for load in loads:
                    load.start()
                for load in loads:
                    load.wait()

            b_copy(s).wait()

            p_v[s % 2] = jnp.dot(a_v[...], b_v[s % BUFFERS], preferred_element_type=jnp.float32)

        @pl.when(valid(s - 1))
        def _():
            b = s - 1
            d_copy(b).wait_recv()
            s1_v[b % SUMS1] = p_v[b % 2, pl.ds(pl.multiple_of(c * half, half), half), :] + rd_v[b % 2]
            d_copy(b).wait_send()

        def add_first(b):
            first_copy(b).wait_recv()
            kept = s1_v[b % SUMS1, pl.ds(pl.multiple_of(f * 2 * rows, 2 * rows), 2 * rows), :]
            s2_v[b % SUMS2] = kept + r1_v[b % SLOTS1]
            first_copy(b).wait_send()

        def add_second(b):
            second_copy(b).wait_recv()
            kept = s2_v[b % SUMS2, pl.ds(pl.multiple_of(g * rows, rows), rows), :]
            part = pl.ds(pl.multiple_of((b % blocks) * COLS, COLS), COLS)
            c_ref[a_rows(b // blocks), part] = (kept + r2_v[b % SLOTS2]).astype(c_ref.dtype)
            second_copy(b).wait_send()

        each(sent(s - 1 - LAG1), sent(s - LAG1), add_first)
        each(sent(s - 2 - LAG1 - HELD2 - LAG2), sent(s - 1 - LAG1 - HELD2 - LAG2), add_second)

    for i in range(len(PEERS)):
        a_sent(i).wait_send()


def solution(mesh):
    def local_product(a_rows, b_rows):
        row_count = a_rows.shape[0]
        k_dim, n_dim = b_rows.shape
        rows = row_count // CHUNKS
        f32, dma = jnp.float32, pltpu.SemaphoreType.DMA
        c_rows, _ = pl.pallas_call(
            kernel,
            name="exchange_matmul",
            out_shape=(
                pltpu.VMEM((row_count, n_dim), jnp.bfloat16),
                jax.ShapeDtypeStruct((8, row_count, k_dim), jnp.bfloat16),
            ),
            in_specs=[pl.BlockSpec(memory_space=pl.ANY)] * 2,
            out_specs=[pl.BlockSpec(memory_space=pltpu.VMEM), pl.BlockSpec(memory_space=pl.ANY)],
            scratch_shapes=[
                pltpu.VMEM((len(PEERS), rows, PIECE), jnp.bfloat16),
                pltpu.VMEM((8 * rows, k_dim), jnp.bfloat16),
                pltpu.VMEM((BUFFERS, k_dim, COLS), jnp.bfloat16),
                pltpu.VMEM((2, 8 * rows, COLS), f32),
                pltpu.VMEM((2, 4 * rows, COLS), f32),
                pltpu.VMEM((SUMS1, 4 * rows, COLS), f32),
                pltpu.VMEM((SLOTS1, 2 * rows, COLS), f32),
                pltpu.VMEM((SUMS2, 2 * rows, COLS), f32),
                pltpu.VMEM((SLOTS2, rows, COLS), f32),
                dma((len(PEERS),)),
                dma((ARRIVING, len(PEERS))),
                dma((len(PEERS) + 1,)),
                dma((BUFFERS,)),
                dma((2,)),
                dma((2,)),
                dma((SENDS1,)),
                dma((SLOTS1,)),
                dma((SENDS2,)),
                dma((SLOTS2,)),
            ],
            compiler_params=pltpu.CompilerParams(
                collective_id=0, has_side_effects=True, vmem_limit_bytes=59 * 1024 * 1024
            ),
            cost_estimate=pl.CostEstimate(
                flops=2 * 8 * row_count * k_dim * n_dim,
                bytes_accessed=2 * CHUNKS * k_dim * n_dim,
                transcendentals=0,
            ),
        )(a_rows, b_rows)
        return c_rows

    return jax.shard_map(
        local_product,
        mesh=mesh,
        in_specs=(P(("mp", "dp"), None), P(("mp", "dp"), None)),
        out_specs=P(("mp", "dp"), None),
        check_vma=False,
    )
```
